256 devices in a mesh: wide: 64 (over y, z_lo, x), layer: 4 (over z_hi, core).
Axes of the slice: x: 4, y: 4, z: 8 (z_hi: 2, z_lo: 4; z = z_hi * 4 + z_lo), core: 2. Of those that a mesh axis runs over, the one named last changes fastest.
Arguments:
- factor: float32 [32768, 8192], P('layer', 'wide'), parts along dimension 0, may hold values from -1 to 21, as said below
Outputs:
- rotated: float32 [32768, 8192], P('layer', 'wide'), parts along dimension 0
- eigen_basis: float32 [32768, 8192], P('layer', 'wide'), parts along dimension 0
The draws below stay inside these ranges and needn't reach their ends.
There are 4 independent parts, one for each index of `layer`. The reference program is written for one: setup_inputs(seed, part) draws one part's arguments, and reference() takes and returns one part's arrays. A program takes and returns all parts, laid end to end along the dimension named above; each array names one. Nothing has to cross between parts.
Inputs may be any that keep to these rules, and one draw needn't show every extreme that they name: `factor`: symmetric.
All inputs are finite; a program needn't handle non-finite values.
Results may differ from the reference program's by a relative error of at most 0.00095.
Values sent between devices are 32-bit elements; how exact they have to be, the bound alone decides.
A program may use at most 128 MiB of HBM per device.

```python
import jax
import jax.numpy as jnp
from jax import lax

BW = 64
SWEEPS = 3
NN = 8192
N_WIDE = 64


def draw_factor(key, part):
    key_diag, key_noise = jax.random.split(jax.random.fold_in(key, 7), 2)
    diagonal_vals = jnp.exp(jax.random.uniform(key_diag, (NN,), jnp.float32, jnp.log(2.0), jnp.log(20.0)))
    positions = jnp.arange(NN, dtype=jnp.int32)
    block_ids = positions // (2 * BW)
    inside = (block_ids[:, None] == block_ids[None, :]).astype(jnp.float32)
    off_diagonal = (positions[:, None] != positions[None, :]).astype(jnp.float32)
    level = 0.012 + (0.15 - 0.012) * inside
    raw_noise = jax.random.normal(key_noise, (NN, NN), jnp.float32)
    sym_noise = (raw_noise + raw_noise.T) * (level / 1.41421356) * off_diagonal
    sym_noise = jnp.clip(sym_noise, -1.0, 1.0)
    return sym_noise + jnp.diag(diagonal_vals)


def setup_inputs(seed: int = 0, part: int = 0) -> dict:
    splits = jax.random.split(jax.random.key(seed), 2)
    part_splits = jax.random.split(jax.random.fold_in(splits[1], part), 2)
    factor = draw_factor(jax.random.fold_in(jax.random.fold_in(splits[1], part), 71), part)
    return dict(factor=factor)


floor_term = 0.01

def cayley_sweeps(pair_block):
    order_size = pair_block.shape[0]
    identity_mat = jnp.eye(order_size, dtype=pair_block.dtype)
    rotation = identity_mat
    for repeat in range(SWEEPS):
        diagonal = jnp.diagonal(pair_block)
        spread = diagonal[None, :] - diagonal[:, None]
        ratios = pair_block * spread / (spread * spread + 2.0 * pair_block * pair_block + floor_term)
        skewed = 0.5 * (ratios - ratios.T) * (1.0 - identity_mat)
        half_turn = identity_mat + 0.5 * skewed
        system = identity_mat - 0.25 * jnp.dot(skewed, skewed, precision=lax.Precision.HIGHEST)
        lower_part = jnp.linalg.cholesky(system)
        square_turn = jnp.dot(half_turn, half_turn, precision=lax.Precision.HIGHEST)
        rotate_now = jax.scipy.linalg.cho_solve((lower_part, True), square_turn)
        pair_block = jnp.dot(rotate_now.T, jnp.dot(pair_block, rotate_now, precision=lax.Precision.HIGHEST), precision=lax.Precision.HIGHEST)
        rotation = jnp.dot(rotation, rotate_now, precision=lax.Precision.HIGHEST)
    return rotation

def trade_blocks(array, axis_num):
    moved = jnp.moveaxis(array, axis_num, 0)
    rest_shape = moved.shape[1:]
    split_view = moved.reshape((2, N_WIDE // 2, 2, BW) + rest_shape)
    joined = jnp.concatenate([split_view[:, :, :1], split_view[::-1, :, 1:]], axis=2)
    return jnp.moveaxis(joined.reshape(moved.shape), 0, axis_num)

def reference(factor):
    pair_span = 2 * BW
    current = factor
    basis = jnp.eye(NN, dtype=factor.dtype)
    index_list = jnp.arange(N_WIDE)
    for repeat in range(2):
        if repeat == 1:
            current = trade_blocks(trade_blocks(current, 0), 1)
            basis = trade_blocks(basis, 1)
        grid = current.reshape(N_WIDE, pair_span, N_WIDE, pair_span)
        diagonal_blocks = grid[index_list, :, index_list, :]
        turns = lax.map(cayley_sweeps, diagonal_blocks)
        columns = jnp.einsum('kald,ldc->kalc', grid, turns, precision=lax.Precision.HIGHEST)
        updated = jnp.einsum('kba,kblc->kalc', turns, columns, precision=lax.Precision.HIGHEST)
        current = updated.reshape(NN, NN)
        basis_view = basis.reshape(NN, N_WIDE, pair_span)
        basis = jnp.einsum('ild,ldc->ilc', basis_view, turns, precision=lax.Precision.HIGHEST).reshape(NN, NN)
    return (current, basis)
```

```python
import functools

import jax
import jax.numpy as jnp
from jax import lax
from jax.experimental import pallas as pl
from jax.experimental.pallas import tpu as pltpu
from jax.sharding import PartitionSpec as P

SWEEPS = 3
f32, bf16 = jnp.float32, jnp.bfloat16
floor_term = 0.01
HBM = pl.BlockSpec(memory_space=pl.ANY)
VMEM = pl.BlockSpec(memory_space=pltpu.VMEM)


def dot(a, b):
    return jnp.dot(a, b, precision=lax.Precision.HIGHEST, preferred_element_type=f32)


def split(a):
    high = a.astype(bf16)
    return high, (a - high.astype(f32)).astype(bf16)


def paired(b):
    high, low = split(b)
    return jnp.concatenate(
        [
            jnp.concatenate([high, low], axis=1),
            jnp.concatenate([high, jnp.zeros_like(low)], axis=1),
        ],
        axis=0,
    )


def dot_paired(a, b_paired):
    both = jnp.dot(jnp.concatenate(split(a), axis=1), b_paired, preferred_element_type=f32)
    half = both.shape[1] // 2
    return both[:, :half] + both[:, half:]


def dot_three(a, b):
    return dot_paired(a, paired(b))


def rotation(block):
    size = block.shape[0]
    row = lax.broadcasted_iota(jnp.int32, (size, size), 0)
    eye = (row == lax.broadcasted_iota(jnp.int32, (size, size), 1)).astype(f32)

    def sweep(_, carry):
        m, q = carry
        on = m * eye
        spread = jnp.sum(on, axis=0, keepdims=True) - jnp.sum(on, axis=1, keepdims=True)
        ratio = m * spread / (spread * spread + 2.0 * m * m + floor_term)
        k = 0.5 * (ratio - ratio.T)
        square = dot(k, k)
        bound = jnp.sum(jnp.abs(square), axis=0, keepdims=True)
        bound = 0.25 * 1.001 * jnp.max(bound, axis=1, keepdims=True)
        scale = 2.0 / (2.0 + bound)
        reach = bound / (2.0 + bound)
        e = eye * (1.0 - scale) + (0.25 * scale) * square
        p = 2.0 * scale * eye + scale * k

        def step(c):
            p, e, reach, _ = c
            w = 2.0 / (2.0 - reach * reach)
            both = dot_three(jnp.concatenate([p, e], axis=0), e)
            reach = reach * reach / (2.0 - reach * reach)
            return w * (p + both[:size]), eye * (1.0 - w) + w * both[size:], reach, jnp.max(reach)

        p, *_ = lax.while_loop(lambda c: c[3] > 1e-7, step, (p, e, reach, jnp.max(reach)))
        rest = 2.0 * eye - p + 0.5 * dot(k, p)
        g = p + 0.5 * dot_three(p, rest) - eye
        both = dot(jnp.concatenate([m, q], axis=0), g)
        return dot(g.T, both[:size]), both[size:]

    return lax.fori_loop(0, SWEEPS, sweep, (block, eye))


def my_rows(span):
    return pl.ds(pl.multiple_of(lax.axis_index("wide") * span, span), span)


def first_kernel(whole_ref, block_ref, q_ref, note_ref, send_ref, keep_ref, m_ref, w_ref, sem):
    span = q_ref.shape[0]
    half = span // 2

    @pl.when(pl.program_id(0) == 0)
    def _():
        copy = pltpu.make_async_copy(whole_ref.at[my_rows(span)], m_ref, sem)
        copy.start()
        copy.wait()
        m, q = rotation(m_ref[...])
        q_ref[...] = q
        note_ref[:half] = q.T[half:]
        note_ref[half:] = m[half:]
        m_ref[...] = m
        w_ref[0] = paired(jnp.concatenate([q[:, half:], q[:, :half]], axis=1))
        w_ref[1] = paired(q)

    top = dot_paired(block_ref[0], w_ref[0])
    bottom = dot_paired(block_ref[1], w_ref[1])
    low = lax.broadcasted_iota(jnp.int32, top.shape, 1) < half
    send_ref[...] = jnp.where(low, top, bottom)
    keep_ref[...] = jnp.where(low, bottom, top)


def first_round(factor, rows):
    order, span = factor.shape
    square = jax.ShapeDtypeStruct((span, span), f32)
    packed = jax.ShapeDtypeStruct((order // 2, span), f32)
    fixed = pl.BlockSpec((span, span), lambda i: (0, 0))
    moving = pl.BlockSpec((rows, span), lambda i: (i, 0))
    return pl.pallas_call(
        first_kernel,
        grid=(order // 2 // rows,),
        out_shape=(square, square, packed, packed, square),
        in_specs=[HBM, pl.BlockSpec((2, rows, span), lambda i: (0, i, 0))],
        out_specs=[fixed, fixed, moving, moving, fixed],
        scratch_shapes=[
            pltpu.VMEM((2, 2 * span, 2 * span), bf16),
            pltpu.SemaphoreType.DMA,
        ],
        cost_estimate=pl.CostEstimate(flops=3 * 10**9, bytes_accessed=10**7, transcendentals=0),
        name="first_round",
    )(factor, factor.reshape(2, order // 2, span))


def second_kernel(pairs, whole_ref, q_ref, m_ref, note_ref, turn_ref, wt_ref, w_ref, cross_ref, sem):
    span = q_ref.shape[0]
    half = span // 2
    mine = lax.axis_index("wide")
    other = lax.rem(mine + pairs // 2, pairs)
    copy = pltpu.make_async_copy(
        whole_ref.at[pl.ds(pl.multiple_of(other * span, span), span)], cross_ref, sem
    )
    copy.start()
    copy.wait()
    q = q_ref[...]
    qt = q.T
    note = note_ref[...]
    across = dot(note[:half], dot(cross_ref[...], q))[:, :half]
    m = m_ref[...]
    block = jnp.concatenate(
        [
            jnp.concatenate([m[:half, :half], across.T], axis=1),
            jnp.concatenate([across, note[half:, half:]], axis=1),
        ],
        axis=0,
    )
    _, turn = rotation(block)
    turn_ref[...] = turn
    turned = turn.T
    here = dot(turned[:, :half], qt[:half])
    there = dot(turned[:, half:], note[:half])
    low = mine < pairs // 2
    wt_ref[:, :span] = jnp.where(low, here, there)
    wt_ref[:, span:] = jnp.where(low, there, here)
    w_ref[0] = here.T
    w_ref[1] = there.T


def second_round(factor, q, m, note):
    order, span = factor.shape
    return pl.pallas_call(
        functools.partial(second_kernel, order // span),
        out_shape=(
            jax.ShapeDtypeStruct((span, span), f32),
            jax.ShapeDtypeStruct((span, 2 * span), f32),
            jax.ShapeDtypeStruct((2, span, span), f32),
        ),
        in_specs=[HBM, VMEM, VMEM, VMEM],
        out_specs=[VMEM, VMEM, VMEM],
        scratch_shapes=[pltpu.VMEM((span, span), f32), pltpu.SemaphoreType.DMA],
        cost_estimate=pl.CostEstimate(flops=2 * 10**9, bytes_accessed=10**6, transcendentals=0),
        name="second_round",
    )(factor, q, m, note)


def last_kernel(recv_ref, keep_ref, turn_ref, wt_ref, out_ref, turn_pair):
    span = turn_ref.shape[0]
    half = span // 2

    @pl.when(pl.program_id(0) == 0)
    def _():
        turn = turn_ref[...]
        turn_pair[0] = paired(jnp.concatenate([turn[half:], turn[:half]], axis=0))
        turn_pair[1] = paired(turn)

    recv, keep = recv_ref[...], keep_ref[...]
    low = lax.broadcasted_iota(jnp.int32, recv.shape, 1) < half
    top = dot_paired(jnp.where(low, recv, keep), turn_pair[0])
    bottom = dot_paired(jnp.where(low, keep, recv), turn_pair[1])
    for b in range(wt_ref.shape[1]):
        rows = slice(b * span, (b + 1) * span)
        z_high, z_low = split(jnp.concatenate([top[rows], bottom[rows]], axis=0))
        w_high, w_low = split(jnp.concatenate([wt_ref[0, b], wt_ref[1, b]], axis=0))
        both = jnp.dot(
            w_high, jnp.concatenate([z_high, z_low], axis=1), preferred_element_type=f32
        )
        out = both[:, :span] + both[:, span:] + jnp.dot(w_low, z_high, preferred_element_type=f32)
        out_ref[0, rows] = out[:span]
        out_ref[1, rows] = out[span:]


def last_step(recv, keep, turn, wt, at_once):
    rows, span = recv.shape
    rows_now = at_once * span
    moving = pl.BlockSpec((rows_now, span), lambda i: (i, 0))
    out = pl.pallas_call(
        last_kernel,
        grid=(rows // rows_now,),
        out_shape=jax.ShapeDtypeStruct((2, rows, span), f32),
        in_specs=[
            moving,
            moving,
            pl.BlockSpec((span, span), lambda i: (0, 0)),
            pl.BlockSpec((2, at_once, span, 2 * span), lambda i: (0, i, 0, 0)),
        ],
        out_specs=pl.BlockSpec((2, rows_now, span), lambda i: (0, i, 0)),
        scratch_shapes=[pltpu.VMEM((2, 2 * span, 2 * span), bf16)],
        cost_estimate=pl.CostEstimate(flops=3 * 10**9, bytes_accessed=10**7, transcendentals=0),
        name="last_step",
    )(recv, keep, turn, wt.reshape(2, -1, span, 2 * span))
    return out.reshape(2 * rows, span)


def body(pairs, factor):
    order, span = factor.shape
    mine = lax.axis_index("wide")
    other = lax.rem(mine + pairs // 2, pairs)
    partners = [(i, (i + pairs // 2) % pairs) for i in range(pairs)]
    q, note, send, keep, m = first_round(factor, 512)
    note = lax.ppermute(note, "wide", partners)
    recv = lax.ppermute(send, "wide", partners)
    turn, wt, w = second_round(factor, q, m, note)
    basis = jnp.zeros((order, span), f32)
    basis = lax.dynamic_update_slice_in_dim(basis, w[0], mine * span, 0)
    basis = lax.dynamic_update_slice_in_dim(basis, w[1], other * span, 0)
    rotated = last_step(recv, keep, turn, lax.all_gather(wt, "wide"), 2)
    return rotated, basis


def solution(mesh):
    spec = P("layer", "wide")
    return jax.shard_map(
        functools.partial(body, mesh.shape["wide"]),
        mesh=mesh,
        in_specs=(spec,),
        out_specs=(spec, spec),
        check_vma=False,
    )
```

```python
import functools

import jax
import jax.numpy as jnp
from jax import lax
from jax.experimental import pallas as pl
from jax.experimental.pallas import tpu as pltpu
from jax.sharding import PartitionSpec as P

SWEEPS = 3
f32, bf16 = jnp.float32, jnp.bfloat16
floor_term = 0.01
HBM = pl.BlockSpec(memory_space=pl.ANY)
VMEM = pl.BlockSpec(memory_space=pltpu.VMEM)


def dot(a, b):
    return jnp.dot(a, b, precision=lax.Precision.HIGHEST, preferred_element_type=f32)


def split(a):
    high = a.astype(bf16)
    return high, (a - high.astype(f32)).astype(bf16)


def paired(b):
    high, low = split(b)
    return jnp.concatenate(
        [
            jnp.concatenate([high, low], axis=1),
            jnp.concatenate([high, jnp.zeros_like(low)], axis=1),
        ],
        axis=0,
    )


def dot_paired(a, b_paired):
    both = jnp.dot(jnp.concatenate(split(a), axis=1), b_paired, preferred_element_type=f32)
    half = both.shape[1] // 2
    return both[:, :half] + both[:, half:]


def dot_three(a, b):
    return dot_paired(a, paired(b))


def rotation(block, steps=None):
    size = block.shape[0]
    row = lax.broadcasted_iota(jnp.int32, (size, size), 0)
    eye = (row == lax.broadcasted_iota(jnp.int32, (size, size), 1)).astype(f32)

    def sweep(_, carry):
        m, q = carry
        on = m * eye
        spread = jnp.sum(on, axis=0, keepdims=True) - jnp.sum(on, axis=1, keepdims=True)
        ratio = m * spread / (spread * spread + 2.0 * m * m + floor_term)
        k = 0.5 * (ratio - ratio.T)
        square = dot(k, k)
        bound = jnp.sum(jnp.abs(square), axis=0, keepdims=True)
        bound = 0.25 * 1.001 * jnp.max(bound, axis=1, keepdims=True)
        scale = 2.0 / (2.0 + bound)
        reach = bound / (2.0 + bound)
        e = eye * (1.0 - scale) + (0.25 * scale) * square
        p = 2.0 * scale * eye + scale * k

        def step(p, e, reach):
            w = 2.0 / (2.0 - reach * reach)
            both = dot_three(jnp.concatenate([p, e], axis=0), e)
            reach = reach * reach / (2.0 - reach * reach)
            return w * (p + both[:size]), eye * (1.0 - w) + w * both[size:], reach

        if steps is None:
            p, *_ = lax.while_loop(
                lambda c: c[3] > 1e-4,
                lambda c: (lambda n: (*n, jnp.max(n[2])))(step(*c[:3])),
                (p, e, reach, jnp.max(reach)),
            )
        else:
            p, *_ = lax.fori_loop(0, steps, lambda _, c: step(*c), (p, e, reach))
        rest = 2.0 * eye - p + 0.5 * dot(k, p)
        g = p + 0.5 * dot_three(p, rest) - eye
        both = dot(jnp.concatenate([m, q], axis=0), g)
        return dot(g.T, both[:size]), both[size:]

    return lax.fori_loop(0, SWEEPS, sweep, (block, eye))


def rows_at(index, span):
    return pl.ds(pl.multiple_of(index * span, span), span)


def first_kernel(
    a_ref, q_ref, qt_ref, note_ref, m_ref, send_ref, keep_ref, zero_ref,
    a_held, send_held, keep_held, zeros, w_ref, in_sem, out_sem, zero_sem,
):
    span = q_ref.shape[0]
    half = span // 2
    order = a_ref.shape[0]
    rows = zeros.shape[0]
    tiles = order // 2 // rows
    mine = rows_at(lax.axis_index("wide"), span)
    pair = pltpu.make_async_copy(a_ref.at[mine], m_ref, in_sem.at[0])
    pair.start()
    whole = pltpu.make_async_copy(a_ref, a_held, in_sem.at[1])
    whole.start()
    zeros[...] = jnp.zeros_like(zeros)
    cleared = [
        pltpu.make_async_copy(zeros, zero_ref.at[pl.ds(i * rows, rows)], zero_sem.at[i])
        for i in range(2 * tiles)
    ]
    pair.wait()
    m, q = rotation(m_ref[...])
    q_ref[...] = q
    qt = q.T
    qt_ref[...] = qt
    note_ref[:half] = qt[half:]
    note_ref[half:] = m[half:]
    m_ref[...] = m
    for copy in cleared:
        copy.start()
    w_ref[0] = paired(jnp.concatenate([q[:, half:], q[:, :half]], axis=1))
    w_ref[1] = paired(q)
    whole.wait()
    out = []
    for i in range(tiles):
        upper, lower = pl.ds(i * rows, rows), pl.ds(order // 2 + i * rows, rows)
        top = dot_paired(a_held[upper], w_ref[0])
        bottom = dot_paired(a_held[lower], w_ref[1])
        low = lax.broadcasted_iota(jnp.int32, top.shape, 1) < half
        send_held[upper] = jnp.where(low, top, bottom)
        keep_held[upper] = jnp.where(low, bottom, top)
        for n, (held, ref) in enumerate(((send_held, send_ref), (keep_held, keep_ref))):
            out.append(pltpu.make_async_copy(held.at[upper], ref.at[upper], out_sem.at[n, i]))
            out[-1].start()
    for copy in out + cleared:
        copy.wait()


def first_round(factor, rows):
    order, span = factor.shape
    square = jax.ShapeDtypeStruct((span, span), f32)
    packed = jax.ShapeDtypeStruct((order // 2, span), f32)
    tiles = order // 2 // rows
    return pl.pallas_call(
        first_kernel,
        out_shape=(
            square, square, square, square, packed, packed,
            jax.ShapeDtypeStruct((order, span), f32),
        ),
        in_specs=[HBM],
        out_specs=[VMEM] * 4 + [HBM] * 3,
        scratch_shapes=[
            pltpu.VMEM((order, span), f32),
            pltpu.VMEM((order // 2, span), f32),
            pltpu.VMEM((order // 2, span), f32),
            pltpu.VMEM((rows, span), f32),
            pltpu.VMEM((2, 2 * span, 2 * span), bf16),
            pltpu.SemaphoreType.DMA((2,)),
            pltpu.SemaphoreType.DMA((2, tiles)),
            pltpu.SemaphoreType.DMA((2 * tiles,)),
        ],
        compiler_params=pltpu.CompilerParams(vmem_limit_bytes=62 * 2**20),
        cost_estimate=pl.CostEstimate(flops=3 * 10**9, bytes_accessed=10**7, transcendentals=0),
        name="first_round",
    )(factor)


def along(axis, step):
    me = lax.axis_index("wide")
    weight = {"y": 16, "z": 4, "x": 1}[axis]
    place = lax.rem(me // weight, 4)
    return me + (lax.rem(place + step + 4, 4) - place) * weight


def remote(src, dst, sems, at, target):
    return pltpu.make_async_remote_copy(
        src_ref=src,
        dst_ref=dst,
        send_sem=sems.at[(0, *at)],
        recv_sem=sems.at[(1, *at)],
        device_id={"wide": target},
        device_id_type=pl.DeviceIdType.MESH,
    )


class Gather:
    def __init__(self, buf, ring_sems, x_sems):
        self.buf, self.ring, self.ends = buf, ring_sems, x_sems
        me = lax.axis_index("wide")
        self.y, self.z, self.x = lax.rem(me // 16, 4), lax.rem(me // 4, 4), lax.rem(me, 4)
        self.sent = []

    def start(self, src, dst, sems, at, target):
        copy = remote(src, dst, sems, at, target)
        copy.start()
        self.sent.append(copy)

    def arrived(self, place, sems, at):
        remote(place, place, sems, at, lax.axis_index("wide")).wait_recv()

    def y_start(self, src):
        place = self.buf.at[self.x, self.z, self.y]
        for i in (1, 3, 2):
            self.start(src, place, self.ring, (0, i), along("y", i))

    def y_wait(self):
        for i in (1, 3, 2):
            y = lax.rem(self.y - i + 4, 4)
            self.arrived(self.buf.at[self.x, self.z, y], self.ring, (0, i))

    def z_start(self):
        place = self.buf.at[self.x, self.z]
        for i in (1, 3, 2):
            self.start(place, place, self.ring, (1, i), along("z", i))

    def plane(self, i):
        return lax.rem(self.z - i + 4, 4)

    def z_wait(self, i):
        self.arrived(self.buf.at[self.x, self.plane(i)], self.ring, (1, i))

    def x_start(self, i):
        place = self.buf.at[self.x, self.plane(i)]
        self.start(place, place, self.ends, (0, i), along("x", 1))
        self.start(place, place, self.ends, (1, i), along("x", 3))

    def x_forward(self, i):
        for way, step in ((0, 3), (1, 1)):
            source = lax.rem(self.x + step, 4)
            place = self.buf.at[source, self.plane(i)]
            self.arrived(place, self.ends, (way, i))
            part = self.buf.at[source, self.plane(i), pl.ds(2 * way, 2)]
            self.start(part, part, self.ends, (2 + way, i), along("x", 4 - step))

    def x_wait(self, i):
        source = lax.rem(self.x + 2, 4)
        for way in (0, 1):
            part = self.buf.at[source, self.plane(i), pl.ds(2 * way, 2)]
            self.arrived(part, self.ends, (2 + way, i))

    def drain(self):
        for copy in self.sent:
            copy.wait_send()


def round_kernel(
    pieces, a_ref, q_ref, qt_ref, m_ref, note_ref, send_ref, keep_ref,
    out_ref, w_ref,
    first, second, recv, keep, z_ref, turn_pair, cross, note, turned_ref,
    local_sem, note_sem, bulk_sem, ring_one, ends_one, ring_two, ends_two,
):
    span = q_ref.shape[0]
    half = span // 2
    pairs = a_ref.shape[0] // span
    mine = lax.axis_index("wide")
    partner = along("y", 2)
    barrier = pltpu.get_barrier_semaphore()
    peers = [("y", 1), ("y", 2), ("y", 3), ("z", 1), ("z", 2), ("z", 3), ("x", 1), ("x", 3)]
    for axis, step in peers:
        pl.semaphore_signal(
            barrier, inc=1, device_id={"wide": along(axis, step)},
            device_id_type=pl.DeviceIdType.MESH,
        )
    x, z, y = lax.rem(mine, 4), lax.rem(mine // 4, 4), lax.rem(mine // 16, 4)
    local = [
        pltpu.make_async_copy(a_ref.at[rows_at(partner, span)], cross, local_sem.at[0]),
        pltpu.make_async_copy(qt_ref, first.at[x, z, y], local_sem.at[1]),
        pltpu.make_async_copy(keep_ref, keep, local_sem.at[2]),
    ]
    for copy in local:
        copy.start()
    pl.semaphore_wait(barrier, len(peers))

    told = remote(note_ref, note, note_sem, (), partner)
    told.start()
    one, two = Gather(first, ring_one, ends_one), Gather(second, ring_two, ends_two)
    one.y_start(qt_ref)
    size = send_ref.shape[0] // pieces
    bulk = [
        remote(send_ref.at[pl.ds(i * size, size)], recv.at[pl.ds(i * size, size)], bulk_sem, (i,), partner)
        for i in range(pieces)
    ]
    early = pieces // 2
    for copy in bulk[:early]:
        copy.start()
    local[1].wait()
    one.y_wait()
    one.z_start()
    one.x_start(0)

    local[0].wait()
    told.wait_recv()
    q = q_ref[...]
    across = dot(note[:half], dot(cross[...], q))[:, :half]
    m = m_ref[...]
    block = jnp.concatenate(
        [
            jnp.concatenate([m[:half, :half], across.T], axis=1),
            jnp.concatenate([across, note[half:, half:]], axis=1),
        ],
        axis=0,
    )
    _, turn = rotation(block, 8)
    turned = turn.T
    turned_ref[...] = turned
    w_ref[0] = dot(qt_ref[:half].T, turn[:half])
    w_ref[1] = dot(note[:half].T, turn[half:])
    turn_pair[0] = paired(jnp.concatenate([turn[half:], turn[:half]], axis=0))
    turn_pair[1] = paired(turn)
    second[x, z, y] = turned
    two.y_start(turned_ref)
    for copy in bulk[early:]:
        copy.start()
    for i in (1, 3, 2):
        one.z_wait(i)
        one.x_start(i)
    one.x_forward(0)
    two.y_wait()
    two.z_start()
    for i in (1, 3, 2):
        one.x_forward(i)
    two.x_start(0)
    for i in (1, 3, 2):
        two.z_wait(i)
        two.x_start(i)
    for i in (0, 1, 3, 2):
        one.x_wait(i)

    local[2].wait()
    for copy in bulk:
        copy.wait_recv()
    low = lax.broadcasted_iota(jnp.int32, (span, span), 1) < half

    def near(n, carry):
        at = rows_at(n, span)
        got, held = recv[at], keep[at]
        place = (lax.rem(n, 4), lax.rem(n // 4, 4))
        top = dot_paired(jnp.where(low, got, held), turn_pair[0])
        bottom = dot_paired(jnp.where(low, held, got), turn_pair[1])
        upper = dot_three(first[(*place, n // 16)], top)
        lower = dot_three(first[(*place, n // 16 + 2)], bottom)
        z_ref[0, at] = jnp.concatenate([upper[:half], lower[half:]], axis=0)
        z_ref[1, at] = jnp.concatenate([lower[:half], upper[half:]], axis=0)
        return carry

    lax.fori_loop(0, pairs // 2, near, 0)

    def far(x_at, z_at):
        for b in range(2):
            at = rows_at(16 * b + 4 * z_at + x_at, span)
            for side in range(2):
                out_ref[side, at] = dot_three(second[x_at, z_at, b + 2 * side], z_ref[side, at])

    for i in (0, 1, 3, 2):
        two.x_forward(i)
        for step in (0, 1, 3):
            far(lax.rem(x + step, 4), two.plane(i))
    for i in (0, 1, 3, 2):
        two.x_wait(i)
        far(lax.rem(x + 2, 4), two.plane(i))
    told.wait_send()
    for copy in bulk:
        copy.wait_send()
    one.drain()
    two.drain()


def rounds(factor, q, qt, m, note, send, keep, pieces):
    order, span = factor.shape
    gathered = pltpu.VMEM((4, 4, 4, span, span), f32)
    packed = pltpu.VMEM((order // 2, span), f32)
    square = pltpu.VMEM((span, span), f32)
    ring, ends = pltpu.SemaphoreType.DMA((2, 2, 4)), pltpu.SemaphoreType.DMA((2, 4, 4))
    return pl.pallas_call(
        functools.partial(round_kernel, pieces),
        out_shape=(
            jax.ShapeDtypeStruct((2, order // 2, span), f32),
            jax.ShapeDtypeStruct((2, span, span), f32),
        ),
        in_specs=[HBM, VMEM, VMEM, VMEM, VMEM, HBM, HBM],
        out_specs=[VMEM, VMEM],
        scratch_shapes=[
            gathered, gathered, packed, packed,
            pltpu.VMEM((2, order // 2, span), f32),
            pltpu.VMEM((2, 2 * span, 2 * span), bf16),
            square, square, square,
            pltpu.SemaphoreType.DMA((3,)),
            pltpu.SemaphoreType.DMA((2,)),
            pltpu.SemaphoreType.DMA((2, pieces)),
            ring, ends, ring, ends,
        ],
        compiler_params=pltpu.CompilerParams(
            collective_id=0, has_side_effects=True, vmem_limit_bytes=62 * 2**20
        ),
        cost_estimate=pl.CostEstimate(flops=10**10, bytes_accessed=10**7, transcendentals=0),
        name="rounds",
    )(factor, q, qt, m, note, send, keep)


def body(pairs, factor):
    order, span = factor.shape
    mine = lax.axis_index("wide")
    other = lax.rem(mine + pairs // 2, pairs)
    q, qt, note, m, send, keep, basis = first_round(factor, 512)
    rotated, w = rounds(factor, q, qt, m, note, send, keep, 8)
    basis = lax.dynamic_update_slice_in_dim(basis, w[0], mine * span, 0)
    basis = lax.dynamic_update_slice_in_dim(basis, w[1], other * span, 0)
    return rotated.reshape(order, span), basis


def solution(mesh):
    spec = P("layer", "wide")
    return jax.shard_map(
        functools.partial(body, mesh.shape["wide"]),
        mesh=mesh,
        in_specs=(spec,),
        out_specs=(spec, spec),
        check_vma=False,
    )
```

```python
import jax
import jax.numpy as jnp
from jax import lax
from jax.experimental import pallas as pl
from jax.experimental.pallas import tpu as pltpu
from jax.sharding import PartitionSpec as P

SWEEPS = 3
f32, bf16 = jnp.float32, jnp.bfloat16
floor_term = 0.01
HBM = pl.BlockSpec(memory_space=pl.ANY)
VMEM = pl.BlockSpec(memory_space=pltpu.VMEM)


def dot(a, b):
    return jnp.dot(a, b, precision=lax.Precision.HIGHEST, preferred_element_type=f32)


def split(a):
    high = a.astype(bf16)
    return high, (a - high.astype(f32)).astype(bf16)


def paired(b):
    high, low = split(b)
    return jnp.concatenate(
        [
            jnp.concatenate([high, low], axis=1),
            jnp.concatenate([high, jnp.zeros_like(low)], axis=1),
        ],
        axis=0,
    )


def dot_paired(a, b_paired):
    both = jnp.dot(jnp.concatenate(split(a), axis=1), b_paired, preferred_element_type=f32)
    half = both.shape[1] // 2
    return both[:, :half] + both[:, half:]


def dot_three(a, b):
    return dot_paired(a, paired(b))


def rotation(block, steps=None, between=None):
    size = block.shape[0]
    row = lax.broadcasted_iota(jnp.int32, (size, size), 0)
    eye = (row == lax.broadcasted_iota(jnp.int32, (size, size), 1)).astype(f32)

    def sweep(_, carry):
        m, q = carry
        on = m * eye
        spread = jnp.sum(on, axis=0, keepdims=True) - jnp.sum(on, axis=1, keepdims=True)
        ratio = m * spread / (spread * spread + 2.0 * m * m + floor_term)
        k = 0.5 * (ratio - ratio.T)
        square = dot(k, k)
        bound = jnp.sum(jnp.abs(square), axis=0, keepdims=True)
        bound = 0.25 * 1.001 * jnp.max(bound, axis=1, keepdims=True)
        scale = 2.0 / (2.0 + bound)
        reach = bound / (2.0 + bound)
        e = eye * (1.0 - scale) + (0.25 * scale) * square
        p = 2.0 * scale * eye + scale * k

        def step(p, e, reach):
            w = 2.0 / (2.0 - reach * reach)
            both = dot_three(jnp.concatenate([p, e], axis=0), e)
            reach = reach * reach / (2.0 - reach * reach)
            return w * (p + both[:size]), eye * (1.0 - w) + w * both[size:], reach

        if steps is None:
            p, *_ = lax.while_loop(
                lambda c: c[3] > 1e-4,
                lambda c: (lambda n: (*n, jnp.max(n[2])))(step(*c[:3])),
                (p, e, reach, jnp.max(reach)),
            )
        else:
            p, *_ = lax.fori_loop(0, steps, lambda _, c: step(*c), (p, e, reach))
        rest = 2.0 * eye - p + 0.5 * dot(k, p)
        g = p + 0.5 * dot_three(p, rest) - eye
        both = dot(jnp.concatenate([m, q], axis=0), g)
        return dot(g.T, both[:size]), both[size:]

    if between is None:
        return lax.fori_loop(0, SWEEPS, sweep, (block, eye))
    carry = (block, eye)
    for repeat in range(SWEEPS):
        carry = sweep(repeat, carry)
        between(repeat)
    return carry


def rows_at(index, span):
    return pl.ds(pl.multiple_of(index * span, span), span)


def first_kernel(a_ref, q_ref, qt_ref, note_ref, m_ref, zero_ref, zeros, in_sem, zero_sem):
    span = q_ref.shape[0]
    half = span // 2
    rows = zeros.shape[0]
    mine = rows_at(lax.axis_index("wide"), span)
    pair = pltpu.make_async_copy(a_ref.at[mine], m_ref, in_sem)
    pair.start()
    zeros[...] = jnp.zeros_like(zeros)
    cleared = [
        pltpu.make_async_copy(zeros, zero_ref.at[pl.ds(i * rows, rows)], zero_sem.at[i])
        for i in range(zero_ref.shape[0] // rows)
    ]
    pair.wait()
    for copy in cleared:
        copy.start()
    m, q = rotation(m_ref[...])
    q_ref[...] = q
    qt = q.T
    qt_ref[...] = qt
    note_ref[:half] = qt[half:]
    note_ref[half:] = m[half:]
    m_ref[...] = m
    for copy in cleared:
        copy.wait()


def first_round(factor, rows):
    order, span = factor.shape
    square = jax.ShapeDtypeStruct((span, span), f32)
    return pl.pallas_call(
        first_kernel,
        out_shape=(square, square, square, square, jax.ShapeDtypeStruct((order, span), f32)),
        in_specs=[HBM],
        out_specs=[VMEM] * 4 + [HBM],
        scratch_shapes=[
            pltpu.VMEM((rows, span), f32),
            pltpu.SemaphoreType.DMA,
            pltpu.SemaphoreType.DMA((order // rows,)),
        ],
        compiler_params=pltpu.CompilerParams(vmem_limit_bytes=62 * 2**20),
        cost_estimate=pl.CostEstimate(flops=10**9, bytes_accessed=10**7, transcendentals=0),
        name="first_round",
    )(factor)


WEIGHT = {"y": 16, "z": 4, "x": 1}


def along(axis, step):
    me = lax.axis_index("wide")
    place = lax.rem(me // WEIGHT[axis], 4)
    return me + (lax.rem(place + step + 4, 4) - place) * WEIGHT[axis]


def remote(src, dst, send_sem, recv_sem, target):
    return pltpu.make_async_remote_copy(
        src_ref=src,
        dst_ref=dst,
        send_sem=send_sem,
        recv_sem=recv_sem,
        device_id={"wide": target},
        device_id_type=pl.DeviceIdType.MESH,
    )


class Gather:
    def __init__(self, buf, y_sems, z_send, z_recv, x_sems):
        self.buf, self.y_sems, self.x_sems = buf, y_sems, x_sems
        self.z_send, self.z_recv = z_send, z_recv
        self.me = lax.axis_index("wide")
        self.y, self.z, self.x = (lax.rem(self.me // WEIGHT[a], 4) for a in "yzx")
        self.sent, self.sent_if = [], []

    def start(self, src, dst, sems, at, target):
        copy = remote(src, dst, sems.at[(0, *at)], sems.at[(1, *at)], target)
        copy.start()
        self.sent.append(copy)

    def arrived(self, place, recv_sem):
        remote(place, place, recv_sem, recv_sem, self.me).wait_recv()

    def y_start(self, src):
        place = self.at(self.x, self.z, self.y)
        for i in (1, 3, 2):
            self.start(src, place, self.y_sems, (i,), along("y", i))

    def y_wait(self):
        for i in (1, 3, 2):
            y = lax.rem(self.y - i + 4, 4)
            self.arrived(self.at(self.x, self.z, y), self.y_sems.at[1, i])

    def plane(self, r):
        far = self.z // 2
        return (self.z, self.z + 1 - 2 * lax.rem(self.z, 2), 2 - far, 3 - 3 * far)[r]

    def z_move(self, condition, plane, slot, to):
        place = self.z_block(plane)
        target = self.me + (to - self.z) * WEIGHT["z"]
        copy = remote(place, place, self.z_send.at[slot], self.z_recv.at[plane], target)
        pl.when(condition)(copy.start)
        self.sent_if.append((condition, copy))

    def z_start(self):
        self.z_move(self.z < 3, self.z, 0, lax.rem(self.z + 1, 4))
        self.z_move(self.z > 0, self.z, 1, lax.rem(self.z + 3, 4))

    def z_take(self, r):
        plane = self.plane(r)
        self.arrived(self.z_block(plane), self.z_recv.at[plane])
        inner = lax.rem(self.z + 1, 4) // 2 == 1
        to = 3 - self.z if r == 1 else 3 * lax.rem(self.z + 3, 4)
        self.z_move(inner, plane, 1 + r, lax.rem(to, 4))

    def x_start(self, r):
        for way, step in ((0, 1), (1, 3)):
            for turn in range(2):
                part = self.at(self.x, self.plane(r), pl.ds(2 * ((way + turn) % 2), 2))
                self.start(part, part, self.x_sems, (2 * way + turn, r), along("x", step))

    def x_forward(self, r):
        for way, step in ((0, 3), (1, 1)):
            part = self.at(lax.rem(self.x + step, 4), self.plane(r), pl.ds(2 * way, 2))
            self.arrived(part, self.x_sems.at[1, 2 * way, r])
            self.start(part, part, self.x_sems, (4 + way, r), along("x", 4 - step))

    def x_near(self, r):
        for way, step in ((0, 3), (1, 1)):
            part = self.at(lax.rem(self.x + step, 4), self.plane(r), pl.ds(2 - 2 * way, 2))
            self.arrived(part, self.x_sems.at[1, 2 * way + 1, r])

    def x_far(self, r):
        for way in (0, 1):
            part = self.at(lax.rem(self.x + 2, 4), self.plane(r), pl.ds(2 * way, 2))
            self.arrived(part, self.x_sems.at[1, 4 + way, r])

    def drain(self):
        for copy in self.sent:
            copy.wait_send()
        for condition, copy in self.sent_if:
            pl.when(condition)(copy.wait_send)
        self.sent, self.sent_if = [], []


class RingLast(Gather):
    def at(self, x, z, *y):
        return self.buf.at[(x, z, *y)]

    def z_block(self, z):
        return self.buf.at[self.x, z]


class LineLast(Gather):
    def at(self, x, z, *y):
        return self.buf.at[(z, x, *y)]

    def z_block(self, z):
        return self.buf.at[z]


GATHER_SEMS = [
    pltpu.SemaphoreType.DMA((2, 4)),
    pltpu.SemaphoreType.DMA((5,)),
    pltpu.SemaphoreType.DMA((4,)),
    pltpu.SemaphoreType.DMA((2, 6, 4)),
]


def round_kernel(
    a_ref, q_ref, qt_ref, m_ref, note_ref,
    out_ref, w_ref,
    first, second, third, held, send, recv, keep, z_ref, q_pair, turn_pair, note, upper_ref, lower_ref,
    local_sem, note_sem, bulk_sem, *gather_sems,
):
    span = q_ref.shape[0]
    half = span // 2
    cut = upper_ref.shape[0]
    order = a_ref.shape[0]
    pairs = order // span
    partner = along("y", 2)
    barrier = pltpu.get_barrier_semaphore()
    peers = [("y", 1), ("y", 2), ("y", 3), ("z", 1), ("z", 3), ("x", 1), ("x", 3)]
    for axis, step in peers:
        pl.semaphore_signal(
            barrier, inc=1, device_id={"wide": along(axis, step)},
            device_id_type=pl.DeviceIdType.MESH,
        )
    one = RingLast(first, *gather_sems[:4])
    two = RingLast(second, *gather_sems[4:8])
    three = LineLast(third, *gather_sems[8:])
    x, z, y = one.x, one.z, one.y
    mine = pltpu.make_async_copy(qt_ref, first.at[x, z, y], local_sem.at[0])
    mine.start()
    whole = pltpu.make_async_copy(a_ref, held, local_sem.at[1])
    whole.start()
    q = q_ref[...]
    q_pair[0] = paired(jnp.concatenate([q[:, half:], q[:, :half]], axis=1))
    q_pair[1] = paired(q)
    pl.semaphore_wait(barrier, len(peers))
    told = remote(note_ref, note, note_sem.at[0], note_sem.at[1], partner)
    told.start()
    one.y_start(qt_ref)

    whole.wait()
    size = 4 * span
    low = lax.broadcasted_iota(jnp.int32, (size, span), 1) < half

    def halves(i, carry):
        at = rows_at(i, size)
        top = dot_paired(held[at], q_pair[0])
        bottom = dot_paired(held[rows_at(i + pairs // 8, size)], q_pair[1])
        send[at] = jnp.where(low, top, bottom)
        keep[at] = jnp.where(low, bottom, top)
        return carry

    lax.fori_loop(0, pairs // 8, halves, 0)
    across = dot(held[rows_at(partner, span)], q)
    bulk = []
    for r in range(4):
        for b in range(2):
            at = rows_at(4 * b + one.plane(r), size)
            sems = (bulk_sem.at[0, r, b], bulk_sem.at[1, r, b])
            bulk.append(remote(send.at[at], recv.at[at], *sems, partner))
    for copy in bulk[:2]:
        copy.start()
    told.wait_recv()
    across = dot(note[:half], across)[:, :half]
    m = m_ref[...]
    block = jnp.concatenate(
        [
            jnp.concatenate([m[:half, :half], across.T], axis=1),
            jnp.concatenate([across, note[half:, half:]], axis=1),
        ],
        axis=0,
    )
    mine.wait()
    one.y_wait()
    one.z_start()
    one.x_start(0)

    def between(repeat):
        if repeat == 1:
            one.x_forward(0)
        if repeat == 2:
            one.z_take(1)
            one.x_start(1)

    _, turn = rotation(block, 7, between)
    turned = turn.T
    upper_ref[...] = turned[:cut]
    lower_ref[...] = turned[cut:]
    second[x, z, y] = turned[:cut]
    third[z, x, y] = turned[cut:]
    turn_pair[0] = paired(jnp.concatenate([turn[half:], turn[:half]], axis=0))
    turn_pair[1] = paired(turn)
    three.y_start(lower_ref)
    two.y_start(upper_ref)
    w_ref[0] = dot(qt_ref[:half].T, turn[:half])
    w_ref[1] = dot(note[:half].T, turn[half:])
    low = low[:span]

    def near(r):
        for copy in bulk[2 * r : 2 * r + 2]:
            copy.wait_recv()
        z_at = one.plane(r)

        def each(t, carry):
            n = 16 * (t // 4) + 4 * z_at + lax.rem(t, 4)
            at = rows_at(n, span)
            got, kept = recv[at], keep[at]
            group = first.at[lax.rem(t, 4), z_at]
            top = dot_paired(jnp.where(low, got, kept), turn_pair[0])
            bottom = dot_paired(jnp.where(low, kept, got), turn_pair[1])
            upper = dot_three(group[t // 4], top)
            lower = dot_three(group[t // 4 + 2], bottom)
            z_ref[0, n] = paired(jnp.concatenate([upper[:half], lower[half:]], axis=0))
            z_ref[1, n] = paired(jnp.concatenate([lower[:half], upper[half:]], axis=0))
            return carry

        lax.fori_loop(0, 8, each, 0)

    def far(group, start, count, x_at, z_at):
        for b in range(2):
            n = 16 * b + 4 * z_at + x_at
            at = pl.ds(pl.multiple_of(n * span, span) + start, count)
            for side in range(2):
                out_ref[side, at] = dot_paired(group[b + 2 * side], z_ref[side, n])

    def far_ring(r, steps):
        for step in steps:
            x_at, z_at = lax.rem(x + step, 4), two.plane(r)
            far(second.at[x_at, z_at], 0, cut, x_at, z_at)

    def far_line(r):
        for step in range(4):
            x_at, z_at = lax.rem(x + step, 4), three.plane(r)
            far(third.at[z_at, x_at], cut, span - cut, x_at, z_at)

    three.drain()
    two.drain()
    for copy in bulk[2:]:
        copy.start()
    three.y_wait()
    three.x_start(0)
    two.y_wait()
    two.z_start()
    one.x_forward(1)
    one.z_take(2)
    one.x_start(2)
    one.x_near(0)
    one.x_far(0)
    near(0)
    three.x_forward(0)
    two.x_start(0)
    one.z_take(3)
    one.x_start(3)
    one.x_forward(2)
    three.x_near(0)
    three.x_far(0)
    three.z_start()
    two.z_take(1)
    two.x_start(1)
    two.x_forward(0)
    one.x_near(1)
    one.x_far(1)
    near(1)
    two.z_take(2)
    two.x_start(2)
    one.x_forward(3)
    three.z_take(1)
    one.x_near(2)
    one.x_far(2)
    near(2)
    two.z_take(3)
    two.x_start(3)
    two.x_forward(1)
    three.z_take(2)
    one.x_near(3)
    one.x_far(3)
    near(3)
    two.x_forward(2)
    far_line(0)
    far_ring(0, (0,))
    two.x_near(0)
    far_ring(0, (1, 3))
    three.z_take(3)
    two.x_forward(3)
    two.x_far(0)
    far_ring(0, (2,))
    for r in (1, 2):
        far_line(r)
        two.x_near(r)
        two.x_far(r)
        far_ring(r, range(4))
    far_line(3)
    two.x_near(3)
    far_ring(3, (0, 1, 3))
    two.x_far(3)
    far_ring(3, (2,))
    told.wait_send()
    for copy in bulk:
        copy.wait_send()
    for gather in (one, two, three):
        gather.drain()


def rounds(factor, q, qt, m, note, cut):
    order, span = factor.shape
    packed = pltpu.VMEM((order // 2, span), f32)
    square = pltpu.VMEM((span, span), f32)
    pair = pltpu.VMEM((2, 2 * span, 2 * span), bf16)
    return pl.pallas_call(
        round_kernel,
        out_shape=(
            jax.ShapeDtypeStruct((2, order // 2, span), f32),
            jax.ShapeDtypeStruct((2, span, span), f32),
        ),
        in_specs=[HBM, VMEM, VMEM, VMEM, VMEM],
        out_specs=[VMEM, VMEM],
        scratch_shapes=[
            pltpu.VMEM((4, 4, 4, span, span), f32),
            pltpu.VMEM((4, 4, 4, cut, span), f32),
            pltpu.VMEM((4, 4, 4, span - cut, span), f32),
            pltpu.VMEM((order, span), f32),
            packed, packed, packed,
            pltpu.VMEM((2, order // span // 2, 2 * span, 2 * span), bf16),
            pair, pair, square,
            pltpu.VMEM((cut, span), f32),
            pltpu.VMEM((span - cut, span), f32),
            pltpu.SemaphoreType.DMA((2,)),
            pltpu.SemaphoreType.DMA((2,)),
            pltpu.SemaphoreType.DMA((2, 4, 2)),
            *(GATHER_SEMS * 3),
        ],
        compiler_params=pltpu.CompilerParams(
            collective_id=0, has_side_effects=True, vmem_limit_bytes=62 * 2**20
        ),
        cost_estimate=pl.CostEstimate(flops=10**10, bytes_accessed=10**7, transcendentals=0),
        name="rounds",
    )(factor, q, qt, m, note)


def finish_kernel(rotated_ref, w_ref, zero_ref, out_ref, basis_ref, held, in_sem, out_sem, w_sem):
    del zero_ref
    pairs = basis_ref.shape[0] // w_ref.shape[1]
    mine = lax.axis_index("wide")
    places = (mine, lax.rem(mine + pairs // 2, pairs))
    tiles = in_sem.shape[0]
    rows = held.shape[0] // tiles
    parts = [pl.ds(i * rows, rows) for i in range(tiles)]
    taken = [
        pltpu.make_async_copy(rotated_ref.at[p], held.at[p], in_sem.at[i])
        for i, p in enumerate(parts)
    ]
    put = [
        pltpu.make_async_copy(held.at[p], out_ref.at[p], out_sem.at[i])
        for i, p in enumerate(parts)
    ]
    for copy in taken:
        copy.start()
    blocks = [
        pltpu.make_async_copy(w_ref.at[i], basis_ref.at[rows_at(p, w_ref.shape[1])], w_sem.at[i])
        for i, p in enumerate(places)
    ]
    for copy in blocks:
        copy.start()
    for got, sent in zip(taken, put):
        got.wait()
        sent.start()
    for copy in put + blocks:
        copy.wait()


def finish(rotated, w, basis, tiles):
    order, span = basis.shape
    shape = jax.ShapeDtypeStruct((order, span), f32)
    return pl.pallas_call(
        finish_kernel,
        out_shape=(shape, shape),
        in_specs=[HBM, VMEM, HBM],
        out_specs=[HBM, HBM],
        input_output_aliases={2: 1},
        scratch_shapes=[
            pltpu.VMEM((order, span), f32),
            pltpu.SemaphoreType.DMA((tiles,)),
            pltpu.SemaphoreType.DMA((tiles,)),
            pltpu.SemaphoreType.DMA((2,)),
        ],
        compiler_params=pltpu.CompilerParams(vmem_limit_bytes=62 * 2**20),
        cost_estimate=pl.CostEstimate(flops=10**6, bytes_accessed=10**7, transcendentals=0),
        name="finish",
    )(rotated, w, basis)


def body(factor):
    q, qt, note, m, basis = first_round(factor, 512)
    rotated, w = rounds(factor, q, qt, m, note, 88)
    return finish(rotated.reshape(factor.shape), w, basis, 8)


def solution(mesh):
    spec = P("layer", "wide")
    return jax.shard_map(
        body,
        mesh=mesh,
        in_specs=(spec,),
        out_specs=(spec, spec),
        check_vma=False,
    )
```

```python
import jax
import jax.numpy as jnp
from jax import lax
from jax.experimental import pallas as pl
from jax.experimental.pallas import tpu as pltpu
from jax.sharding import PartitionSpec as P

SWEEPS = 3
f32, bf16 = jnp.float32, jnp.bfloat16
floor_term = 0.01
HBM = pl.BlockSpec(memory_space=pl.ANY)
VMEM = pl.BlockSpec(memory_space=pltpu.VMEM)


def dot(a, b):
    return jnp.dot(a, b, precision=lax.Precision.HIGHEST, preferred_element_type=f32)


def split(a):
    high = a.astype(bf16)
    return high, (a - high.astype(f32)).astype(bf16)


def paired(b):
    high, low = split(b)
    return jnp.concatenate(
        [
            jnp.concatenate([high, low], axis=1),
            jnp.concatenate([high, jnp.zeros_like(low)], axis=1),
        ],
        axis=0,
    )


def dot_paired(a, b_paired):
    both = jnp.dot(jnp.concatenate(split(a), axis=1), b_paired, preferred_element_type=f32)
    half = both.shape[1] // 2
    return both[:, :half] + both[:, half:]


def dot_three(a, b):
    return dot_paired(a, paired(b))


def rotation(block, steps=None, between=None):
    size = block.shape[0]
    row = lax.broadcasted_iota(jnp.int32, (size, size), 0)
    eye = (row == lax.broadcasted_iota(jnp.int32, (size, size), 1)).astype(f32)

    def sweep(_, carry):
        m, q = carry
        on = m * eye
        spread = jnp.sum(on, axis=0, keepdims=True) - jnp.sum(on, axis=1, keepdims=True)
        ratio = m * spread / (spread * spread + 2.0 * m * m + floor_term)
        k = 0.5 * (ratio - ratio.T)
        square = dot(k, k)
        bound = jnp.sum(jnp.abs(square), axis=0, keepdims=True)
        bound = 0.25 * 1.001 * jnp.max(bound, axis=1, keepdims=True)
        scale = 2.0 / (2.0 + bound)
        reach = bound / (2.0 + bound)
        e = eye * (1.0 - scale) + (0.25 * scale) * square
        p = 2.0 * scale * eye + scale * k

        def step(p, e, reach):
            w = 2.0 / (2.0 - reach * reach)
            both = dot_three(jnp.concatenate([p, e], axis=0), e)
            reach = reach * reach / (2.0 - reach * reach)
            return w * (p + both[:size]), eye * (1.0 - w) + w * both[size:], reach

        if steps is None:
            p, *_ = lax.while_loop(
                lambda c: c[3] > 1e-4,
                lambda c: (lambda n: (*n, jnp.max(n[2])))(step(*c[:3])),
                (p, e, reach, jnp.max(reach)),
            )
        else:
            p, *_ = lax.fori_loop(0, steps, lambda _, c: step(*c), (p, e, reach))
        rest = 2.0 * eye - p + 0.5 * dot(k, p)
        g = p + 0.5 * dot_three(p, rest) - eye
        both = dot(jnp.concatenate([m, q], axis=0), g)
        return dot(g.T, both[:size]), both[size:]

    if between is None:
        return lax.fori_loop(0, SWEEPS, sweep, (block, eye))
    carry = (block, eye)
    for repeat in range(SWEEPS):
        carry = sweep(repeat, carry)
        between(repeat)
    return carry


def rows_at(index, span):
    return pl.ds(pl.multiple_of(index * span, span), span)


def first_kernel(a_ref, q_ref, qt_ref, note_ref, m_ref, zero_ref, zeros, in_sem, zero_sem):
    span = q_ref.shape[0]
    half = span // 2
    rows = zeros.shape[0]
    mine = rows_at(lax.axis_index("wide"), span)
    pair = pltpu.make_async_copy(a_ref.at[mine], m_ref, in_sem)
    pair.start()
    zeros[...] = jnp.zeros_like(zeros)
    cleared = [
        pltpu.make_async_copy(zeros, zero_ref.at[pl.ds(i * rows, rows)], zero_sem.at[i])
        for i in range(zero_ref.shape[0] // rows)
    ]
    pair.wait()
    for copy in cleared:
        copy.start()
    m, q = rotation(m_ref[...])
    q_ref[...] = q
    qt = q.T
    qt_ref[...] = qt
    note_ref[:half] = qt[half:]
    note_ref[half:] = m[half:]
    m_ref[...] = m
    for copy in cleared:
        copy.wait()


def first_round(factor, rows):
    order, span = factor.shape
    square = jax.ShapeDtypeStruct((span, span), f32)
    return pl.pallas_call(
        first_kernel,
        out_shape=(square, square, square, square, jax.ShapeDtypeStruct((order, span), f32)),
        in_specs=[HBM],
        out_specs=[VMEM] * 4 + [HBM],
        scratch_shapes=[
            pltpu.VMEM((rows, span), f32),
            pltpu.SemaphoreType.DMA,
            pltpu.SemaphoreType.DMA((order // rows,)),
        ],
        compiler_params=pltpu.CompilerParams(vmem_limit_bytes=62 * 2**20),
        cost_estimate=pl.CostEstimate(flops=10**9, bytes_accessed=10**7, transcendentals=0),
        name="first_round",
    )(factor)


WEIGHT = {"y": 16, "z": 4, "x": 1}


def along(axis, step):
    me = lax.axis_index("wide")
    place = lax.rem(me // WEIGHT[axis], 4)
    return me + (lax.rem(place + step + 4, 4) - place) * WEIGHT[axis]


def remote(src, dst, send_sem, recv_sem, target):
    return pltpu.make_async_remote_copy(
        src_ref=src,
        dst_ref=dst,
        send_sem=send_sem,
        recv_sem=recv_sem,
        device_id={"wide": target},
        device_id_type=pl.DeviceIdType.MESH,
    )


class Gather:
    def __init__(self, buf, y_sems, z_send, z_recv, x_sems):
        self.buf, self.y_sems, self.x_sems = buf, y_sems, x_sems
        self.z_send, self.z_recv = z_send, z_recv
        self.me = lax.axis_index("wide")
        self.y, self.z, self.x = (lax.rem(self.me // WEIGHT[a], 4) for a in "yzx")
        self.sent, self.sent_if = [], []

    def start(self, src, dst, sems, at, target):
        copy = remote(src, dst, sems.at[(0, *at)], sems.at[(1, *at)], target)
        copy.start()
        self.sent.append(copy)

    def arrived(self, place, recv_sem):
        remote(place, place, recv_sem, recv_sem, self.me).wait_recv()

    def y_start(self, src):
        place = self.at(self.x, self.z, self.y)
        for i in (1, 3, 2):
            self.start(src, place, self.y_sems, (i,), along("y", i))

    def y_wait(self):
        for i in (1, 3, 2):
            y = lax.rem(self.y - i + 4, 4)
            self.arrived(self.at(self.x, self.z, y), self.y_sems.at[1, i])

    def plane(self, r):
        far = self.z // 2
        return (self.z, self.z + 1 - 2 * lax.rem(self.z, 2), 2 - far, 3 - 3 * far)[r]

    def z_move(self, condition, plane, slot, to):
        place = self.z_block(plane)
        target = self.me + (to - self.z) * WEIGHT["z"]
        copy = remote(place, place, self.z_send.at[slot], self.z_recv.at[plane], target)
        pl.when(condition)(copy.start)
        self.sent_if.append((condition, copy))

    def z_start(self):
        self.z_move(self.z < 3, self.z, 0, lax.rem(self.z + 1, 4))
        self.z_move(self.z > 0, self.z, 1, lax.rem(self.z + 3, 4))

    def z_take(self, r):
        self.z_relay(r)
        self.z_end(r)

    def z_relay(self, r):
        plane = self.plane(r)
        inner = lax.rem(self.z + 1, 4) // 2 == 1
        pl.when(inner)(lambda: self.arrived(self.z_block(plane), self.z_recv.at[plane]))
        to = 3 - self.z if r == 1 else 3 * lax.rem(self.z + 3, 4)
        self.z_move(inner, plane, 1 + r, lax.rem(to, 4))

    def z_end(self, r):
        plane = self.plane(r)
        end = lax.rem(self.z + 1, 4) // 2 == 0
        pl.when(end)(lambda: self.arrived(self.z_block(plane), self.z_recv.at[plane]))

    def x_start(self, r):
        for way, step in ((0, 1), (1, 3)):
            for turn in range(2):
                part = self.at(self.x, self.plane(r), pl.ds(2 * ((way + turn) % 2), 2))
                self.start(part, part, self.x_sems, (2 * way + turn, r), along("x", step))

    def x_forward(self, r):
        for way, step in ((0, 3), (1, 1)):
            part = self.at(lax.rem(self.x + step, 4), self.plane(r), pl.ds(2 * way, 2))
            self.arrived(part, self.x_sems.at[1, 2 * way, r])
            self.start(part, part, self.x_sems, (4 + way, r), along("x", 4 - step))

    def x_near(self, r):
        for way, step in ((0, 3), (1, 1)):
            part = self.at(lax.rem(self.x + step, 4), self.plane(r), pl.ds(2 - 2 * way, 2))
            self.arrived(part, self.x_sems.at[1, 2 * way + 1, r])

    def x_far(self, r):
        for way in (0, 1):
            part = self.at(lax.rem(self.x + 2, 4), self.plane(r), pl.ds(2 * way, 2))
            self.arrived(part, self.x_sems.at[1, 4 + way, r])

    def drain(self):
        for copy in self.sent:
            copy.wait_send()
        for condition, copy in self.sent_if:
            pl.when(condition)(copy.wait_send)
        self.sent, self.sent_if = [], []


class RingLast(Gather):
    def at(self, x, z, *y):
        return self.buf.at[(x, z, *y)]

    def z_block(self, z):
        return self.buf.at[self.x, z]


class LineLast(Gather):
    def at(self, x, z, *y):
        return self.buf.at[(z, x, *y)]

    def z_block(self, z):
        return self.buf.at[z]


GATHER_SEMS = [
    pltpu.SemaphoreType.DMA((2, 4)),
    pltpu.SemaphoreType.DMA((5,)),
    pltpu.SemaphoreType.DMA((4,)),
    pltpu.SemaphoreType.DMA((2, 6, 4)),
]


def round_kernel(
    a_ref, q_ref, qt_ref, m_ref, note_ref,
    out_ref, w_ref,
    first, second, third, held, send, recv, keep, z_ref, q_pair, turn_pair, note, upper_ref, lower_ref,
    local_sem, note_sem, bulk_sem, ready_sem, *gather_sems,
):
    span = q_ref.shape[0]
    half = span // 2
    cut = upper_ref.shape[0]
    order = a_ref.shape[0]
    pairs = order // span
    partner = along("y", 2)
    barrier = pltpu.get_barrier_semaphore()
    peers = [("y", 1), ("y", 2), ("y", 3), ("z", 1), ("z", 3), ("x", 1), ("x", 3)]
    for axis, step in peers:
        pl.semaphore_signal(
            barrier, inc=1, device_id={"wide": along(axis, step)},
            device_id_type=pl.DeviceIdType.MESH,
        )
    one = RingLast(first, *gather_sems[:4])
    two = RingLast(second, *gather_sems[4:8])
    three = LineLast(third, *gather_sems[8:])
    x, z, y = one.x, one.z, one.y
    mine = pltpu.make_async_copy(qt_ref, first.at[x, z, y], local_sem.at[0])
    mine.start()
    whole = pltpu.make_async_copy(a_ref, held, local_sem.at[1])
    whole.start()
    q = q_ref[...]
    q_pair[0] = paired(jnp.concatenate([q[:, half:], q[:, :half]], axis=1))
    q_pair[1] = paired(q)
    pl.semaphore_wait(barrier, len(peers))
    told = remote(note_ref, note, note_sem.at[0], note_sem.at[1], partner)
    told.start()
    one.y_start(qt_ref)

    whole.wait()
    size = 4 * span
    low = lax.broadcasted_iota(jnp.int32, (size, span), 1) < half

    def halves(i, carry):
        at = rows_at(i, size)
        top = dot_paired(held[at], q_pair[0])
        bottom = dot_paired(held[rows_at(i + pairs // 8, size)], q_pair[1])
        send[at] = jnp.where(low, top, bottom)
        keep[at] = jnp.where(low, bottom, top)
        return carry

    lax.fori_loop(0, pairs // 8, halves, 0)
    across = dot(held[rows_at(partner, span)], q)
    bulk = []
    for r in range(4):
        for b in range(2):
            at = rows_at(4 * b + one.plane(r), size)
            sems = (bulk_sem.at[0, r, b], bulk_sem.at[1, r, b])
            bulk.append(remote(send.at[at], recv.at[at], *sems, partner))
    for copy in bulk[:2]:
        copy.start()
    told.wait_recv()
    across = dot(note[:half], across)[:, :half]
    m = m_ref[...]
    block = jnp.concatenate(
        [
            jnp.concatenate([m[:half, :half], across.T], axis=1),
            jnp.concatenate([across, note[half:, half:]], axis=1),
        ],
        axis=0,
    )
    mine.wait()
    one.y_wait()
    one.z_start()
    one.x_start(0)

    def between(repeat):
        if repeat == 1:
            one.x_forward(0)
        if repeat == 2:
            one.z_take(1)
            one.x_start(1)

    _, turn = rotation(block, 7, between)
    turned = turn.T
    upper_ref[...] = turned[:cut]
    lower_ref[...] = turned[cut:]
    second[x, z, y] = turned[:cut]
    third[z, x, y] = turned[cut:]
    turn_pair[0] = paired(jnp.concatenate([turn[half:], turn[:half]], axis=0))
    turn_pair[1] = paired(turn)
    three.y_start(lower_ref)
    two.y_start(upper_ref)
    w_ref[0] = dot(qt_ref[:half].T, turn[:half])
    w_ref[1] = dot(note[:half].T, turn[half:])
    low = low[:span]

    def near(r):
        for copy in bulk[2 * r : 2 * r + 2]:
            copy.wait_recv()
        z_at = one.plane(r)

        def each(t, carry):
            n = 16 * (t // 4) + 4 * z_at + lax.rem(t, 4)
            at = rows_at(n, span)
            got, kept = recv[at], keep[at]
            group = first.at[lax.rem(t, 4), z_at]
            top = dot_paired(jnp.where(low, got, kept), turn_pair[0])
            bottom = dot_paired(jnp.where(low, kept, got), turn_pair[1])
            upper = dot_three(group[t // 4], top)
            lower = dot_three(group[t // 4 + 2], bottom)
            z_ref[0, n] = paired(jnp.concatenate([upper[:half], lower[half:]], axis=0))
            z_ref[1, n] = paired(jnp.concatenate([lower[:half], upper[half:]], axis=0))
            return carry

        lax.fori_loop(0, 8, each, 0)

    def far(group, start, count, x_at, z_at):
        for b in range(2):
            n = 16 * b + 4 * z_at + x_at
            at = pl.ds(pl.multiple_of(n * span, span) + start, count)
            for side in range(2):
                out_ref[side, at] = dot_paired(group[b + 2 * side], z_ref[side, n])

    def far_ring(r, steps):
        for step in steps:
            x_at, z_at = lax.rem(x + step, 4), two.plane(r)
            far(second.at[x_at, z_at], 0, cut, x_at, z_at)

    def far_line(r):
        for step in range(4):
            x_at, z_at = lax.rem(x + step, 4), three.plane(r)
            far(third.at[z_at, x_at], cut, span - cut, x_at, z_at)

    three.drain()
    two.drain()
    three.y_wait()
    two.y_wait()
    for step in (1, 2, 3):
        pl.semaphore_signal(
            ready_sem, inc=1, device_id={"wide": along("y", step)},
            device_id_type=pl.DeviceIdType.MESH,
        )
    three.x_start(0)
    two.z_start()
    one.x_forward(1)
    one.z_take(2)
    one.x_start(2)
    one.z_relay(3)
    pl.semaphore_wait(ready_sem, 3)
    for copy in bulk[2:]:
        copy.start()
    one.x_near(0)
    one.x_far(0)
    near(0)
    three.x_forward(0)
    two.x_start(0)
    one.z_end(3)
    one.x_start(3)
    one.x_forward(2)
    three.x_near(0)
    three.x_far(0)
    three.z_start()
    two.z_take(1)
    two.x_start(1)
    two.z_relay(2)
    two.x_forward(0)
    one.x_near(1)
    one.x_far(1)
    near(1)
    two.z_end(2)
    two.x_start(2)
    two.z_relay(3)
    three.z_take(1)
    three.z_relay(2)
    one.x_forward(3)
    one.x_near(2)
    one.x_far(2)
    near(2)
    two.z_end(3)
    two.x_start(3)
    two.x_forward(1)
    one.x_near(3)
    one.x_far(3)
    three.z_relay(3)
    near(3)
    three.z_end(2)
    two.x_forward(2)
    far_line(0)
    far_ring(0, (0,))
    two.x_near(0)
    far_ring(0, (1, 3))
    two.x_forward(3)
    two.x_far(0)
    far_ring(0, (2,))
    for r in (1, 2):
        far_line(r)
        two.x_near(r)
        two.x_far(r)
        far_ring(r, range(4))
    two.x_near(3)
    far_ring(3, (0, 1, 3))
    three.z_end(3)
    far_line(3)
    two.x_far(3)
    far_ring(3, (2,))
    told.wait_send()
    for copy in bulk:
        copy.wait_send()
    for gather in (one, two, three):
        gather.drain()


def rounds(factor, q, qt, m, note, cut):
    order, span = factor.shape
    packed = pltpu.VMEM((order // 2, span), f32)
    square = pltpu.VMEM((span, span), f32)
    pair = pltpu.VMEM((2, 2 * span, 2 * span), bf16)
    return pl.pallas_call(
        round_kernel,
        out_shape=(
            jax.ShapeDtypeStruct((2, order // 2, span), f32),
            jax.ShapeDtypeStruct((2, span, span), f32),
        ),
        in_specs=[HBM, VMEM, VMEM, VMEM, VMEM],
        out_specs=[VMEM, VMEM],
        scratch_shapes=[
            pltpu.VMEM((4, 4, 4, span, span), f32),
            pltpu.VMEM((4, 4, 4, cut, span), f32),
            pltpu.VMEM((4, 4, 4, span - cut, span), f32),
            pltpu.VMEM((order, span), f32),
            packed, packed, packed,
            pltpu.VMEM((2, order // span // 2, 2 * span, 2 * span), bf16),
            pair, pair, square,
            pltpu.VMEM((cut, span), f32),
            pltpu.VMEM((span - cut, span), f32),
            pltpu.SemaphoreType.DMA((2,)),
            pltpu.SemaphoreType.DMA((2,)),
            pltpu.SemaphoreType.DMA((2, 4, 2)),
            pltpu.SemaphoreType.REGULAR,
            *(GATHER_SEMS * 3),
        ],
        compiler_params=pltpu.CompilerParams(
            collective_id=0, has_side_effects=True, vmem_limit_bytes=62 * 2**20
        ),
        cost_estimate=pl.CostEstimate(flops=10**10, bytes_accessed=10**7, transcendentals=0),
        name="rounds",
    )(factor, q, qt, m, note)


def finish_kernel(rotated_ref, w_ref, zero_ref, out_ref, basis_ref, held, in_sem, out_sem, w_sem):
    del zero_ref
    pairs = basis_ref.shape[0] // w_ref.shape[1]
    mine = lax.axis_index("wide")
    places = (mine, lax.rem(mine + pairs // 2, pairs))
    tiles = in_sem.shape[0]
    rows = held.shape[0] // tiles
    parts = [pl.ds(i * rows, rows) for i in range(tiles)]
    taken = [
        pltpu.make_async_copy(rotated_ref.at[p], held.at[p], in_sem.at[i])
        for i, p in enumerate(parts)
    ]
    put = [
        pltpu.make_async_copy(held.at[p], out_ref.at[p], out_sem.at[i])
        for i, p in enumerate(parts)
    ]
    for copy in taken:
        copy.start()
    blocks = [
        pltpu.make_async_copy(w_ref.at[i], basis_ref.at[rows_at(p, w_ref.shape[1])], w_sem.at[i])
        for i, p in enumerate(places)
    ]
    for copy in blocks:
        copy.start()
    for got, sent in zip(taken, put):
        got.wait()
        sent.start()
    for copy in put + blocks:
        copy.wait()


def finish(rotated, w, basis, tiles):
    order, span = basis.shape
    shape = jax.ShapeDtypeStruct((order, span), f32)
    return pl.pallas_call(
        finish_kernel,
        out_shape=(shape, shape),
        in_specs=[HBM, VMEM, HBM],
        out_specs=[HBM, HBM],
        input_output_aliases={2: 1},
        scratch_shapes=[
            pltpu.VMEM((order, span), f32),
            pltpu.SemaphoreType.DMA((tiles,)),
            pltpu.SemaphoreType.DMA((tiles,)),
            pltpu.SemaphoreType.DMA((2,)),
        ],
        compiler_params=pltpu.CompilerParams(vmem_limit_bytes=62 * 2**20),
        cost_estimate=pl.CostEstimate(flops=10**6, bytes_accessed=10**7, transcendentals=0),
        name="finish",
    )(rotated, w, basis)


def body(factor):
    q, qt, note, m, basis = first_round(factor, 512)
    rotated, w = rounds(factor, q, qt, m, note, 80)
    return finish(rotated.reshape(factor.shape), w, basis, 8)


def solution(mesh):
    spec = P("layer", "wide")
    return jax.shard_map(
        body,
        mesh=mesh,
        in_specs=(spec,),
        out_specs=(spec, spec),
        check_vma=False,
    )
```

```python
import jax
import jax.numpy as jnp
from jax import lax
from jax.experimental import pallas as pl
from jax.experimental.pallas import tpu as pltpu
from jax.sharding import PartitionSpec as P

SWEEPS = 3
f32, bf16 = jnp.float32, jnp.bfloat16
floor_term = 0.01
HBM = pl.BlockSpec(memory_space=pl.ANY)
VMEM = pl.BlockSpec(memory_space=pltpu.VMEM)


def dot(a, b):
    return jnp.dot(a, b, precision=lax.Precision.HIGHEST, preferred_element_type=f32)


def split(a):
    high = a.astype(bf16)
    return high, (a - high.astype(f32)).astype(bf16)


def paired(b):
    high, low = split(b)
    return jnp.concatenate(
        [
            jnp.concatenate([high, low], axis=1),
            jnp.concatenate([high, jnp.zeros_like(low)], axis=1),
        ],
        axis=0,
    )


def dot_paired(a, b_paired):
    both = jnp.dot(jnp.concatenate(split(a), axis=1), b_paired, preferred_element_type=f32)
    half = both.shape[1] // 2
    return both[:, :half] + both[:, half:]


def dot_three(a, b):
    return dot_paired(a, paired(b))


def rotation(block, steps=None, between=None):
    size = block.shape[0]
    row = lax.broadcasted_iota(jnp.int32, (size, size), 0)
    eye = (row == lax.broadcasted_iota(jnp.int32, (size, size), 1)).astype(f32)

    def sweep(_, carry):
        m, q = carry
        on = m * eye
        spread = jnp.sum(on, axis=0, keepdims=True) - jnp.sum(on, axis=1, keepdims=True)
        ratio = m * spread / (spread * spread + 2.0 * m * m + floor_term)
        k = 0.5 * (ratio - ratio.T)
        square = dot(k, k)
        bound = jnp.sum(jnp.abs(square), axis=0, keepdims=True)
        bound = 0.25 * 1.001 * jnp.max(bound, axis=1, keepdims=True)
        scale = 2.0 / (2.0 + bound)
        reach = bound / (2.0 + bound)
        e = eye * (1.0 - scale) + (0.25 * scale) * square
        p = 2.0 * scale * eye + scale * k

        def step(p, e, reach):
            w = 2.0 / (2.0 - reach * reach)
            both = dot_three(jnp.concatenate([p, e], axis=0), e)
            reach = reach * reach / (2.0 - reach * reach)
            return w * (p + both[:size]), eye * (1.0 - w) + w * both[size:], reach

        if steps is None:
            p, *_ = lax.while_loop(
                lambda c: c[3] > 1e-4,
                lambda c: (lambda n: (*n, jnp.max(n[2])))(step(*c[:3])),
                (p, e, reach, jnp.max(reach)),
            )
        else:
            p, *_ = lax.fori_loop(0, steps, lambda _, c: step(*c), (p, e, reach))
        rest = 2.0 * eye - p + 0.5 * dot(k, p)
        g = p + 0.5 * dot_three(p, rest) - eye
        both = dot(jnp.concatenate([m, q], axis=0), g)
        return dot(g.T, both[:size]), both[size:]

    if between is None:
        return lax.fori_loop(0, SWEEPS, sweep, (block, eye))
    carry = (block, eye)
    for repeat in range(SWEEPS):
        carry = sweep(repeat, carry)
        between(repeat)
    return carry


def rows_at(index, span):
    return pl.ds(pl.multiple_of(index * span, span), span)


def first_kernel(a_ref, q_ref, qt_ref, note_ref, m_ref, zero_ref, zeros, in_sem, zero_sem):
    span = q_ref.shape[0]
    half = span // 2
    rows = zeros.shape[0]
    mine = rows_at(lax.axis_index("wide"), span)
    pair = pltpu.make_async_copy(a_ref.at[mine], m_ref, in_sem)
    pair.start()
    zeros[...] = jnp.zeros_like(zeros)
    cleared = [
        pltpu.make_async_copy(zeros, zero_ref.at[pl.ds(i * rows, rows)], zero_sem.at[i])
        for i in range(zero_ref.shape[0] // rows)
    ]
    pair.wait()
    for copy in cleared:
        copy.start()
    m, q = rotation(m_ref[...])
    q_ref[...] = q
    qt = q.T
    qt_ref[...] = qt
    note_ref[:half] = qt[half:]
    note_ref[half:] = m[half:]
    m_ref[...] = m
    for copy in cleared:
        copy.wait()


def first_round(factor, rows):
    order, span = factor.shape
    square = jax.ShapeDtypeStruct((span, span), f32)
    return pl.pallas_call(
        first_kernel,
        out_shape=(square, square, square, square, jax.ShapeDtypeStruct((order, span), f32)),
        in_specs=[HBM],
        out_specs=[VMEM] * 4 + [HBM],
        scratch_shapes=[
            pltpu.VMEM((rows, span), f32),
            pltpu.SemaphoreType.DMA,
            pltpu.SemaphoreType.DMA((order // rows,)),
        ],
        compiler_params=pltpu.CompilerParams(vmem_limit_bytes=62 * 2**20),
        cost_estimate=pl.CostEstimate(flops=10**9, bytes_accessed=10**7, transcendentals=0),
        name="first_round",
    )(factor)


WEIGHT = {"y": 16, "z": 4, "x": 1}


def along(axis, step):
    me = lax.axis_index("wide")
    place = lax.rem(me // WEIGHT[axis], 4)
    return me + (lax.rem(place + step + 4, 4) - place) * WEIGHT[axis]


def remote(src, dst, send_sem, recv_sem, target):
    return pltpu.make_async_remote_copy(
        src_ref=src,
        dst_ref=dst,
        send_sem=send_sem,
        recv_sem=recv_sem,
        device_id={"wide": target},
        device_id_type=pl.DeviceIdType.MESH,
    )


class Gather:
    def __init__(self, buf, y_sems, z_send, z_recv, x_sems):
        self.buf, self.y_sems, self.x_sems = buf, y_sems, x_sems
        self.z_send, self.z_recv = z_send, z_recv
        self.me = lax.axis_index("wide")
        self.y, self.z, self.x = (lax.rem(self.me // WEIGHT[a], 4) for a in "yzx")
        self.sent, self.sent_if = [], []

    def start(self, src, dst, sems, at, target):
        copy = remote(src, dst, sems.at[(0, *at)], sems.at[(1, *at)], target)
        copy.start()
        self.sent.append(copy)

    def arrived(self, place, recv_sem):
        remote(place, place, recv_sem, recv_sem, self.me).wait_recv()

    def y_start(self, src):
        place = self.at(self.x, self.z, self.y)
        for i in (1, 3, 2):
            self.start(src, place, self.y_sems, (i,), along("y", i))

    def y_wait(self):
        for i in (1, 3, 2):
            y = lax.rem(self.y - i + 4, 4)
            self.arrived(self.at(self.x, self.z, y), self.y_sems.at[1, i])

    def plane(self, r):
        far = self.z // 2
        return (self.z, self.z + 1 - 2 * lax.rem(self.z, 2), 2 - far, 3 - 3 * far)[r]

    def z_move(self, condition, plane, slot, to):
        place = self.z_block(plane)
        target = self.me + (to - self.z) * WEIGHT["z"]
        copy = remote(place, place, self.z_send.at[slot], self.z_recv.at[plane], target)
        pl.when(condition)(copy.start)
        self.sent_if.append((condition, copy))

    def z_start(self):
        self.z_move(self.z < 3, self.z, 0, lax.rem(self.z + 1, 4))
        self.z_move(self.z > 0, self.z, 1, lax.rem(self.z + 3, 4))

    def z_take(self, r):
        self.z_relay(r)
        self.z_end(r)

    def z_relay(self, r):
        plane = self.plane(r)
        inner = lax.rem(self.z + 1, 4) // 2 == 1
        pl.when(inner)(lambda: self.arrived(self.z_block(plane), self.z_recv.at[plane]))
        to = 3 - self.z if r == 1 else 3 * lax.rem(self.z + 3, 4)
        self.z_move(inner, plane, 1 + r, lax.rem(to, 4))

    def z_end(self, r):
        plane = self.plane(r)
        end = lax.rem(self.z + 1, 4) // 2 == 0
        pl.when(end)(lambda: self.arrived(self.z_block(plane), self.z_recv.at[plane]))

    def x_start(self, r):
        for way, step in ((0, 1), (1, 3)):
            for turn in range(2):
                part = self.at(self.x, self.plane(r), pl.ds(2 * ((way + turn) % 2), 2))
                self.start(part, part, self.x_sems, (2 * way + turn, r), along("x", step))

    def x_forward(self, r):
        for way, step in ((0, 3), (1, 1)):
            part = self.at(lax.rem(self.x + step, 4), self.plane(r), pl.ds(2 * way, 2))
            self.arrived(part, self.x_sems.at[1, 2 * way, r])
            self.start(part, part, self.x_sems, (4 + way, r), along("x", 4 - step))

    def x_near(self, r):
        for way, step in ((0, 3), (1, 1)):
            part = self.at(lax.rem(self.x + step, 4), self.plane(r), pl.ds(2 - 2 * way, 2))
            self.arrived(part, self.x_sems.at[1, 2 * way + 1, r])

    def x_far(self, r):
        for way in (0, 1):
            part = self.at(lax.rem(self.x + 2, 4), self.plane(r), pl.ds(2 * way, 2))
            self.arrived(part, self.x_sems.at[1, 4 + way, r])

    def drain(self):
        for copy in self.sent:
            copy.wait_send()
        for condition, copy in self.sent_if:
            pl.when(condition)(copy.wait_send)
        self.sent, self.sent_if = [], []


class RingLast(Gather):
    def at(self, x, z, *y):
        return self.buf.at[(x, z, *y)]

    def z_block(self, z):
        return self.buf.at[self.x, z]


class LineLast(Gather):
    def at(self, x, z, *y):
        return self.buf.at[(z, x, *y)]

    def z_block(self, z):
        return self.buf.at[z]


GATHER_SEMS = [
    pltpu.SemaphoreType.DMA((2, 4)),
    pltpu.SemaphoreType.DMA((5,)),
    pltpu.SemaphoreType.DMA((4,)),
    pltpu.SemaphoreType.DMA((2, 6, 4)),
]


def round_kernel(
    a_ref, q_ref, qt_ref, m_ref, note_ref,
    put_ref, w_ref,
    out_ref, first, second, third, held, send, recv, keep, z_ref, q_pair, turn_pair, note, upper_ref, lower_ref,
    local_sem, note_sem, bulk_sem, ready_sem, put_sem, *gather_sems,
):
    span = q_ref.shape[0]
    half = span // 2
    cut = upper_ref.shape[0]
    order = a_ref.shape[0]
    pairs = order // span
    partner = along("y", 2)
    barrier = pltpu.get_barrier_semaphore()
    peers = [("y", 1), ("y", 2), ("y", 3), ("z", 1), ("z", 3), ("x", 1), ("x", 3)]
    for axis, step in peers:
        pl.semaphore_signal(
            barrier, inc=1, device_id={"wide": along(axis, step)},
            device_id_type=pl.DeviceIdType.MESH,
        )
    one = RingLast(first, *gather_sems[:4])
    two = RingLast(second, *gather_sems[4:8])
    three = LineLast(third, *gather_sems[8:])
    x, z, y = one.x, one.z, one.y
    mine = pltpu.make_async_copy(qt_ref, first.at[x, z, y], local_sem.at[0])
    mine.start()
    whole = pltpu.make_async_copy(a_ref, held, local_sem.at[1])
    whole.start()
    q = q_ref[...]
    q_pair[0] = paired(jnp.concatenate([q[:, half:], q[:, :half]], axis=1))
    q_pair[1] = paired(q)
    pl.semaphore_wait(barrier, len(peers))
    told = remote(note_ref, note, note_sem.at[0], note_sem.at[1], partner)
    told.start()
    one.y_start(qt_ref)

    whole.wait()
    size = 4 * span
    low = lax.broadcasted_iota(jnp.int32, (size, span), 1) < half

    def halves(i, carry):
        at = rows_at(i, size)
        top = dot_paired(held[at], q_pair[0])
        bottom = dot_paired(held[rows_at(i + pairs // 8, size)], q_pair[1])
        send[at] = jnp.where(low, top, bottom)
        keep[at] = jnp.where(low, bottom, top)
        return carry

    lax.fori_loop(0, pairs // 8, halves, 0)
    across = dot(held[rows_at(partner, span)], q)
    bulk = []
    for r in range(4):
        for b in range(2):
            at = rows_at(4 * b + one.plane(r), size)
            sems = (bulk_sem.at[0, r, b], bulk_sem.at[1, r, b])
            bulk.append(remote(send.at[at], recv.at[at], *sems, partner))
    for copy in bulk[:2]:
        copy.start()
    told.wait_recv()
    across = dot(note[:half], across)[:, :half]
    m = m_ref[...]
    block = jnp.concatenate(
        [
            jnp.concatenate([m[:half, :half], across.T], axis=1),
            jnp.concatenate([across, note[half:, half:]], axis=1),
        ],
        axis=0,
    )
    mine.wait()
    one.y_wait()
    one.z_start()
    one.x_start(0)

    def between(repeat):
        if repeat == 1:
            one.x_forward(0)
        if repeat == 2:
            one.z_take(1)
            one.x_start(1)

    _, turn = rotation(block, 7, between)
    turned = turn.T
    upper_ref[...] = turned[:cut]
    lower_ref[...] = turned[cut:]
    second[x, z, y] = turned[:cut]
    third[z, x, y] = turned[cut:]
    turn_pair[0] = paired(jnp.concatenate([turn[half:], turn[:half]], axis=0))
    turn_pair[1] = paired(turn)
    three.y_start(lower_ref)
    two.y_start(upper_ref)
    w_ref[0] = dot(qt_ref[:half].T, turn[:half])
    w_ref[1] = dot(note[:half].T, turn[half:])
    low = low[:span]

    def near(r):
        for copy in bulk[2 * r : 2 * r + 2]:
            copy.wait_recv()
        z_at = one.plane(r)

        def each(t, carry):
            n = 16 * (t // 4) + 4 * z_at + lax.rem(t, 4)
            at = rows_at(n, span)
            got, kept = recv[at], keep[at]
            group = first.at[lax.rem(t, 4), z_at]
            top = dot_paired(jnp.where(low, got, kept), turn_pair[0])
            bottom = dot_paired(jnp.where(low, kept, got), turn_pair[1])
            upper = dot_three(group[t // 4], top)
            lower = dot_three(group[t // 4 + 2], bottom)
            z_ref[0, n] = paired(jnp.concatenate([upper[:half], lower[half:]], axis=0))
            z_ref[1, n] = paired(jnp.concatenate([lower[:half], upper[half:]], axis=0))
            return carry

        lax.fori_loop(0, 8, each, 0)

    def far(group, start, count, x_at, z_at):
        for b in range(2):
            n = 16 * b + 4 * z_at + x_at
            at = pl.ds(pl.multiple_of(n * span, span) + start, count)
            for side in range(2):
                out_ref[side, at] = dot_paired(group[b + 2 * side], z_ref[side, n])

    def far_ring(r, steps):
        for step in steps:
            x_at, z_at = lax.rem(x + step, 4), two.plane(r)
            far(second.at[x_at, z_at], 0, cut, x_at, z_at)

    def far_line(r):
        for step in range(4):
            x_at, z_at = lax.rem(x + step, 4), three.plane(r)
            far(third.at[z_at, x_at], cut, span - cut, x_at, z_at)

    put = []

    def put_out(r):
        for b in range(2):
            at = rows_at(4 * b + one.plane(r), size)
            for side in range(2):
                copy = pltpu.make_async_copy(
                    out_ref.at[side, at], put_ref.at[side, at], put_sem.at[r, b, side]
                )
                copy.start()
                put.append(copy)

    three.drain()
    two.drain()
    three.y_wait()
    two.y_wait()
    for step in (1, 2, 3):
        pl.semaphore_signal(
            ready_sem, inc=1, device_id={"wide": along("y", step)},
            device_id_type=pl.DeviceIdType.MESH,
        )
    three.x_start(0)
    two.z_start()
    one.x_forward(1)
    one.z_take(2)
    one.x_start(2)
    one.z_relay(3)
    pl.semaphore_wait(ready_sem, 3)
    for copy in bulk[2:]:
        copy.start()
    one.x_near(0)
    one.x_far(0)
    near(0)
    three.x_forward(0)
    two.x_start(0)
    one.z_end(3)
    one.x_start(3)
    one.x_forward(2)
    three.x_near(0)
    three.x_far(0)
    three.z_start()
    two.z_take(1)
    two.x_start(1)
    two.z_relay(2)
    two.x_forward(0)
    one.x_near(1)
    one.x_far(1)
    near(1)
    two.z_end(2)
    two.x_start(2)
    two.z_relay(3)
    three.z_take(1)
    three.z_relay(2)
    one.x_forward(3)
    one.x_near(2)
    one.x_far(2)
    near(2)
    two.z_end(3)
    two.x_start(3)
    two.x_forward(1)
    one.x_near(3)
    one.x_far(3)
    three.z_relay(3)
    near(3)
    three.z_end(2)
    two.x_forward(2)
    far_line(0)
    far_ring(0, (0,))
    two.x_near(0)
    far_ring(0, (1, 3))
    two.x_forward(3)
    two.x_far(0)
    far_ring(0, (2,))
    for r in (1, 2):
        far_line(r)
        two.x_near(r)
        two.x_far(r)
        far_ring(r, range(4))
    for r in (0, 1, 2):
        put_out(r)
    two.x_near(3)
    far_ring(3, (0, 1, 3))
    three.z_end(3)
    far_line(3)
    two.x_far(3)
    far_ring(3, (2,))
    put_out(3)
    for copy in put:
        copy.wait()
    told.wait_send()
    for copy in bulk:
        copy.wait_send()
    for gather in (one, two, three):
        gather.drain()


def rounds(factor, q, qt, m, note, cut):
    order, span = factor.shape
    packed = pltpu.VMEM((order // 2, span), f32)
    square = pltpu.VMEM((span, span), f32)
    pair = pltpu.VMEM((2, 2 * span, 2 * span), bf16)
    return pl.pallas_call(
        round_kernel,
        out_shape=(
            jax.ShapeDtypeStruct((2, order // 2, span), f32),
            jax.ShapeDtypeStruct((2, span, span), f32),
        ),
        in_specs=[HBM, VMEM, VMEM, VMEM, VMEM],
        out_specs=[HBM, VMEM],
        scratch_shapes=[
            pltpu.VMEM((2, order // 2, span), f32),
            pltpu.VMEM((4, 4, 4, span, span), f32),
            pltpu.VMEM((4, 4, 4, cut, span), f32),
            pltpu.VMEM((4, 4, 4, span - cut, span), f32),
            pltpu.VMEM((order, span), f32),
            packed, packed, packed,
            pltpu.VMEM((2, order // span // 2, 2 * span, 2 * span), bf16),
            pair, pair, square,
            pltpu.VMEM((cut, span), f32),
            pltpu.VMEM((span - cut, span), f32),
            pltpu.SemaphoreType.DMA((2,)),
            pltpu.SemaphoreType.DMA((2,)),
            pltpu.SemaphoreType.DMA((2, 4, 2)),
            pltpu.SemaphoreType.REGULAR,
            pltpu.SemaphoreType.DMA((4, 2, 2)),
            *(GATHER_SEMS * 3),
        ],
        compiler_params=pltpu.CompilerParams(
            collective_id=0, has_side_effects=True, vmem_limit_bytes=62 * 2**20
        ),
        cost_estimate=pl.CostEstimate(flops=10**10, bytes_accessed=10**7, transcendentals=0),
        name="rounds",
    )(factor, q, qt, m, note)


def finish_kernel(rotated_ref, w_ref, zero_ref, out_ref, basis_ref, held, in_sem, out_sem, w_sem):
    del zero_ref
    pairs = basis_ref.shape[0] // w_ref.shape[1]
    mine = lax.axis_index("wide")
    places = (mine, lax.rem(mine + pairs // 2, pairs))
    tiles = in_sem.shape[0]
    rows = held.shape[0] // tiles
    parts = [pl.ds(i * rows, rows) for i in range(tiles)]
    taken = [
        pltpu.make_async_copy(rotated_ref.at[p], held.at[p], in_sem.at[i])
        for i, p in enumerate(parts)
    ]
    put = [
        pltpu.make_async_copy(held.at[p], out_ref.at[p], out_sem.at[i])
        for i, p in enumerate(parts)
    ]
    for copy in taken:
        copy.start()
    blocks = [
        pltpu.make_async_copy(w_ref.at[i], basis_ref.at[rows_at(p, w_ref.shape[1])], w_sem.at[i])
        for i, p in enumerate(places)
    ]
    for copy in blocks:
        copy.start()
    for got, sent in zip(taken, put):
        got.wait()
        sent.start()
    for copy in put + blocks:
        copy.wait()


def finish(rotated, w, basis, tiles):
    order, span = basis.shape
    shape = jax.ShapeDtypeStruct((order, span), f32)
    return pl.pallas_call(
        finish_kernel,
        out_shape=(shape, shape),
        in_specs=[HBM, VMEM, HBM],
        out_specs=[HBM, HBM],
        input_output_aliases={2: 1},
        scratch_shapes=[
            pltpu.VMEM((order, span), f32),
            pltpu.SemaphoreType.DMA((tiles,)),
            pltpu.SemaphoreType.DMA((tiles,)),
            pltpu.SemaphoreType.DMA((2,)),
        ],
        compiler_params=pltpu.CompilerParams(vmem_limit_bytes=62 * 2**20),
        cost_estimate=pl.CostEstimate(flops=10**6, bytes_accessed=10**7, transcendentals=0),
        name="finish",
    )(rotated, w, basis)


def body(factor):
    q, qt, note, m, basis = first_round(factor, 512)
    rotated, w = rounds(factor, q, qt, m, note, 72)
    return finish(rotated.reshape(factor.shape), w, basis, 4)


def solution(mesh):
    spec = P("layer", "wide")
    return jax.shard_map(
        body,
        mesh=mesh,
        in_specs=(spec,),
        out_specs=(spec, spec),
        check_vma=False,
    )
```
